32 devices in a mesh: dp: 2 (over x), x: 4 (over z), y: 4 (over y, core).
Axes of the slice: x: 2, y: 2, z: 4, core: 2. Of those that a mesh axis runs over, the one named last changes fastest.
Arguments:
- hidden: bfloat16 [2048, 1024], P('dp', 'x'), parts along dimension 0
- w_qkv: bfloat16 [1024, 3072], P('x', 'y')
- b_qkv: bfloat16 [3072], P('y')
- w_out: bfloat16 [1024, 1024], P('y', 'x')
- b_out: bfloat16 [1024], P('x')
- attn_gain: bfloat16 [1024], P('x')
- attn_shift: bfloat16 [1024], P('x')
- w_up: bfloat16 [1024, 2, 4096], P('x', None, 'y')
- b_up: bfloat16 [2, 4096], P(None, 'y')
- w_down: bfloat16 [4096, 1024], P('y', 'x')
- b_down: bfloat16 [1024], P('x')
- mlp_gain: bfloat16 [1024], P('x')
- mlp_shift: bfloat16 [1024], P('x')
- k_cache: bfloat16 [2048, 64, 16, 64], P('dp', None, 'y'), parts along dimension 0
- v_cache: bfloat16 [2048, 64, 16, 64], P('dp', None, 'y'), parts along dimension 0
- positions: int32 [2048], P('dp'), parts along dimension 0
- lengths: int32 [2048], P('dp'), parts along dimension 0
Outputs:
- output 1: bfloat16 [2048, 1024], P('dp', 'x'), parts along dimension 0
- output 2: bfloat16 [2048, 64, 16, 64], P('dp', None, 'y'), parts along dimension 0
- output 3: bfloat16 [2048, 64, 16, 64], P('dp', None, 'y'), parts along dimension 0
There are 2 independent parts. The reference program is written for one: setup_inputs(seed, part) draws one part's arguments, and reference() takes and returns one part's arrays. A program takes and returns all parts, laid end to end along the dimension named above; an argument that names none is the same for every part.
All inputs are finite; a program needn't handle non-finite values.
Results may differ from the reference program's by a relative error of at most 0.02.
Values are sent between devices in bfloat16 or wider.
A program may use at most 1 GiB of HBM per device.

```python
import math
import jax
import jax.numpy as jnp
from jax import lax

D = 1024
HEADS = 16
HEAD = 64
FF = 4096
BATCH_ROWS = 1024
CACHE_LEN = 64

DEEP_ALPHA = math.sqrt(140.0)
LN_EPS = 1e-5
ROPE_BASE = 10000.0


def setup_inputs(seed: int = 0, part: int = 0) -> dict:
    root_key = jax.random.key(seed)
    weight_keys = jax.random.split(root_key, 12)
    part_keys = jax.random.split(jax.random.fold_in(root_key, part), 5)

    def draw_normal(key, shape, scale):
        return jax.random.normal(key, shape, jnp.float32) * scale

    col_ramp = 0.4 + 1.2 * jnp.arange(D, dtype=jnp.float32) / D
    hidden = (draw_normal(part_keys[0], (BATCH_ROWS, D), 1.0) * col_ramp).astype(jnp.bfloat16)
    w_qkv = draw_normal(weight_keys[0], (D, 3 * D), D ** -0.5).astype(jnp.bfloat16)
    b_qkv = draw_normal(weight_keys[1], (3 * D,), 0.5).astype(jnp.bfloat16)
    w_out = draw_normal(weight_keys[2], (D, D), 2.0 * DEEP_ALPHA * D ** -0.5).astype(jnp.bfloat16)
    b_out = draw_normal(weight_keys[3], (D,), 0.3 * DEEP_ALPHA).astype(jnp.bfloat16)
    attn_gain = (col_ramp * (1.0 + draw_normal(weight_keys[4], (D,), 0.2))).astype(jnp.bfloat16)
    attn_shift = draw_normal(weight_keys[5], (D,), 0.3).astype(jnp.bfloat16)
    w_up = draw_normal(weight_keys[6], (D, 2, FF), D ** -0.5).astype(jnp.bfloat16)
    b_up = draw_normal(weight_keys[7], (2, FF), 0.5).astype(jnp.bfloat16)
    w_down = draw_normal(weight_keys[8], (FF, D), 1.2 * DEEP_ALPHA * FF ** -0.5).astype(jnp.bfloat16)
    b_down = draw_normal(weight_keys[9], (D,), 0.3 * DEEP_ALPHA).astype(jnp.bfloat16)
    mlp_gain = (1.0 + draw_normal(weight_keys[10], (D,), 0.3)).astype(jnp.bfloat16)
    mlp_shift = draw_normal(weight_keys[11], (D,), 0.3).astype(jnp.bfloat16)
    k_cache = draw_normal(part_keys[1], (BATCH_ROWS, CACHE_LEN, HEADS, HEAD), 2.0).astype(jnp.bfloat16)
    v_cache = draw_normal(part_keys[2], (BATCH_ROWS, CACHE_LEN, HEADS, HEAD), 1.0).astype(jnp.bfloat16)
    lengths = jax.random.randint(part_keys[3], (BATCH_ROWS,), 0, CACHE_LEN, jnp.int32)
    lengths = lengths.at[0].set(CACHE_LEN - 1).at[1].set(0)
    offsets = jax.random.randint(part_keys[4], (BATCH_ROWS,), 0, CACHE_LEN, jnp.int32)
    offsets = offsets.at[2].set(CACHE_LEN - 1).at[3].set(0)
    positions = lengths + offsets
    return {'hidden': hidden, 'w_qkv': w_qkv, 'b_qkv': b_qkv, 'w_out': w_out, 'b_out': b_out, 'attn_gain': attn_gain, 'attn_shift': attn_shift, 'w_up': w_up, 'b_up': b_up, 'w_down': w_down, 'b_down': b_down, 'mlp_gain': mlp_gain, 'mlp_shift': mlp_shift, 'k_cache': k_cache, 'v_cache': v_cache, 'positions': positions, 'lengths': lengths}


def apply_rotary(head_vec, positions):
    half_dim = HEAD // 2
    inv_freq = ROPE_BASE ** (-2.0 * jnp.arange(half_dim, dtype=jnp.float32) / HEAD)
    angles = positions.astype(jnp.float32)[:, None] * inv_freq[None, :]
    cos_table = jnp.cos(angles)[:, None, :]
    sin_table = jnp.sin(angles)[:, None, :]
    vec_wide = head_vec.astype(jnp.float32)
    lower_half = vec_wide[..., :half_dim]
    upper_half = vec_wide[..., half_dim:]
    return jnp.concatenate([lower_half * cos_table - upper_half * sin_table, upper_half * cos_table + lower_half * sin_table], axis=-1).astype(jnp.bfloat16)


def layer_norm(h_val, gain, shift):
    mean_row = jnp.mean(h_val, axis=-1, keepdims=True)
    var_row = jnp.mean(jnp.square(h_val - mean_row), axis=-1, keepdims=True)
    return (h_val - mean_row) * lax.rsqrt(var_row + LN_EPS) * gain.astype(jnp.float32) + shift.astype(jnp.float32)


def reference(hidden, w_qkv, b_qkv, w_out, b_out, attn_gain, attn_shift, w_up, b_up, w_down, b_down, mlp_gain, mlp_shift, k_cache, v_cache, positions, lengths):
    qkv_vals = (jnp.dot(hidden, w_qkv, preferred_element_type=jnp.float32) + b_qkv.astype(jnp.float32)).astype(jnp.bfloat16)
    qkv_vals = qkv_vals.reshape(BATCH_ROWS, HEADS, 3, HEAD)
    query_rot = apply_rotary(qkv_vals[:, :, 0], positions)
    key_rot = apply_rotary(qkv_vals[:, :, 1], positions)
    slot_hit = (jnp.arange(CACHE_LEN)[None, :] == lengths[:, None])[:, :, None, None]
    k_full = jnp.where(slot_hit, key_rot[:, None], k_cache)
    v_full = jnp.where(slot_hit, qkv_vals[:, None, :, 2], v_cache)

    def attend_row(row_args):
        query_row, key_row, value_row, length_row = row_args
        scores = jnp.einsum('hd,shd->hs', query_row.astype(jnp.float32), key_row.astype(jnp.float32)) * (HEAD ** -0.5)
        slot_ok = jnp.arange(CACHE_LEN)[None, :] <= length_row
        scores = jnp.where(slot_ok, scores, -1e30)
        attn_probs = jax.nn.softmax(scores, axis=-1).astype(jnp.bfloat16).astype(jnp.float32)
        return jnp.einsum('hs,shd->hd', attn_probs, value_row.astype(jnp.float32)).astype(jnp.bfloat16)

    attn_out = lax.map(attend_row, (query_rot, k_full, v_full, lengths)).reshape(BATCH_ROWS, D)
    proj_sum = jnp.dot(attn_out, w_out, preferred_element_type=jnp.float32) + b_out.astype(jnp.float32)
    h_attn = DEEP_ALPHA * hidden.astype(jnp.float32) + proj_sum
    normed = layer_norm(h_attn, attn_gain, attn_shift).astype(jnp.bfloat16)
    up_sum = jnp.dot(normed, w_up.reshape(D, 2 * FF), preferred_element_type=jnp.float32).reshape(BATCH_ROWS, 2, FF) + b_up.astype(jnp.float32)
    gated_act = (jax.nn.gelu(up_sum[:, 0], approximate=True) * up_sum[:, 1]).astype(jnp.bfloat16)
    down_sum = jnp.dot(gated_act, w_down, preferred_element_type=jnp.float32)
    h_mlp = DEEP_ALPHA * normed.astype(jnp.float32) + down_sum + b_down.astype(jnp.float32)
    result = layer_norm(h_mlp, mlp_gain, mlp_shift).astype(jnp.bfloat16)
    return (result, k_full, v_full)
```

```python
import functools
import math
import jax
import jax.numpy as jnp
from jax import lax
from jax.experimental import pallas as pl
from jax.experimental.pallas import tpu as pltpu
from jax.sharding import PartitionSpec as P

DEEP_ALPHA = math.sqrt(140.0)
LN_EPS = 1e-5
ROPE_BASE = 10000.0
MESH = pl.DeviceIdType.MESH
VMEM = pltpu.VMEM
F32 = jnp.float32
BF16 = jnp.bfloat16


def where_am_i():
    dp, x, y = lax.axis_index("dp"), lax.axis_index("x"), lax.axis_index("y")
    core, chip = lax.rem(y, 2), y // 2
    return dp, x, y, core, chip, core * 2 + chip


def remote(src, dst, send, recv, device):
    return pltpu.make_async_remote_copy(
        src_ref=src, dst_ref=dst, send_sem=send, recv_sem=recv, device_id=device, device_id_type=MESH)


def greet(devices):
    barrier = pltpu.get_barrier_semaphore()
    for device in devices:
        pl.semaphore_signal(barrier, inc=1, device_id=device, device_id_type=MESH)
    pl.semaphore_wait(barrier, len(devices))


def qkv_kernel(hid_ref, w_ref, b_ref, vec_ref, cos_ref, sin_ref,
               q_ref, k_ref, v_ref, hres_ref, vecs_ref,
               hbuf, wbuf, vbuf, hz_s, hz_r, hy_s, hy_r, hd_s, hd_r, wz_s, wz_r, wx_s, wx_r, vz_s, vz_r):
    dp, x, y, core, chip, piece = where_am_i()
    mate = (dp, x, chip * 2 + 1 - core)
    across = (dp, x, (1 - chip) * 2 + core)
    twin = (1 - dp, x, y)
    peers = [(dp, lax.rem(x + j, 4), y) for j in (1, 2, 3)]
    source = [lax.rem(x + 4 - j, 4) for j in (0, 1, 2, 3)]
    greet(peers + [mate, across, twin])

    row0 = pl.multiple_of(piece * 256, 256)
    hz, wz, vz = [], [], []
    for j in (1, 2, 3):
        c = remote(hid_ref.at[pl.ds(row0, 256)], hbuf.at[piece, x], hz_s.at[j], hz_r.at[j], peers[j - 1])
        c.start()
        hz.append(c)
    half0 = pl.multiple_of(dp * 128, 128)
    for j in (1, 2, 3):
        c = remote(w_ref.at[pl.ds(half0, 128)], wbuf.at[x, dp], wz_s.at[j], wz_r.at[j], peers[j - 1])
        c.start()
        wz.append(c)
        c = remote(vec_ref, vbuf.at[x], vz_s.at[j], vz_r.at[j], peers[j - 1])
        c.start()
        vz.append(c)
    for part in range(4):
        hbuf[part, x] = hid_ref[part * 256:(part + 1) * 256, :]
    for half in range(2):
        wbuf[x, half] = w_ref[half * 128:(half + 1) * 128, :]
    vbuf[x] = vec_ref[...]

    hy, hd, wx = [], [], []
    for j in (1, 2, 3):
        hz[j - 1].wait_recv()
        c = remote(hbuf.at[piece, source[j]], hbuf.at[piece, source[j]], hy_s.at[j], hy_r.at[j], across)
        c.start()
        hy.append(c)
    for j in (1, 2, 3):
        hy[j - 1].wait_recv()
        both = hbuf.at[pl.ds(core * 2, 2), source[j]]
        c = remote(both, both, hd_s.at[j], hd_r.at[j], mate)
        c.start()
        hd.append(c)
    for j in (1, 2, 3):
        wz[j - 1].wait_recv()
        block = wbuf.at[source[j], dp]
        c = remote(block, block, wx_s.at[j], wx_r.at[j], twin)
        c.start()
        wx.append(c)
    for c in hd + vz + wx:
        c.wait_recv()

    for s in range(4):
        hres_ref[:, s * 256:(s + 1) * 256] = hbuf[x, s, pl.ds(pl.multiple_of(piece * 64, 64), 64), :]
        vecs_ref[:, s * 256:(s + 1) * 256] = vbuf[s]

    def rows(part, _):
        acc = jnp.dot(hbuf[part, 0], wbuf[0].reshape(256, 768), preferred_element_type=F32)
        for s in (1, 2, 3):
            acc += jnp.dot(hbuf[part, s], wbuf[s].reshape(256, 768), preferred_element_type=F32)
        acc = (acc + b_ref[...].astype(F32)).astype(BF16).astype(F32)
        lanes = pl.ds(pl.multiple_of(part * 256, 256), 256)
        cos, sin = cos_ref[:, lanes], sin_ref[:, lanes]
        acc = acc.T
        for head in range(4):
            base = head * 192
            for off, ref in ((0, q_ref), (64, k_ref)):
                low, high = acc[base + off:base + off + 32], acc[base + off + 32:base + off + 64]
                ref[head * 64:head * 64 + 32, lanes] = (low * cos - high * sin).astype(BF16)
                ref[head * 64 + 32:head * 64 + 64, lanes] = (high * cos + low * sin).astype(BF16)
            v_ref[head * 64:(head + 1) * 64, lanes] = acc[base + 128:base + 192].astype(BF16)
        return 0

    lax.fori_loop(0, 4, rows, 0)
    for c in hz + wz + vz + hy + hd + wx:
        c.wait_send()


def cache_kernel(len_ref, q_ref, kn_ref, vn_ref, k_ref, v_ref, ko_ref, vo_ref, attn_ref, sc_ref):
    slots = k_ref.shape[0]
    lens = len_ref[...]
    k_new, v_new = kn_ref[...], vn_ref[...]
    mine = pl.program_id(0) == lax.axis_index("x")

    def hit(s):
        return jnp.broadcast_to((lens - s).astype(F32), k_new.shape).astype(BF16) == 0

    @pl.when(jnp.logical_not(mine))
    def _():
        def body(s, _):
            m = hit(s)
            ko_ref[s, 0] = jnp.where(m, k_new, k_ref[s, 0])
            vo_ref[s, 0] = jnp.where(m, v_new, v_ref[s, 0])
            return 0
        lax.fori_loop(0, slots, body, 0, unroll=4)
        attn_ref[...] = jnp.zeros_like(attn_ref)

    @pl.when(mine)
    def _():
        q = q_ref[...].astype(F32)

        def keys(s, _):
            kk = jnp.where(hit(s), k_new, k_ref[s, 0])
            ko_ref[s, 0] = kk
            sc_ref[pl.ds(s, 1), :] = jnp.sum(kk.astype(F32) * q, axis=0, keepdims=True)
            return 0
        lax.fori_loop(0, slots, keys, 0, unroll=4)
        sc = sc_ref[...] * (64 ** -0.5)
        sc = jnp.where(lax.broadcasted_iota(jnp.int32, sc.shape, 0) <= lens, sc, -1e30)
        e = jnp.exp(sc - jnp.max(sc, axis=0, keepdims=True))
        sc_ref[...] = (e / jnp.sum(e, axis=0, keepdims=True)).astype(BF16).astype(F32)

        def values(s, acc):
            vv = jnp.where(hit(s), v_new, v_ref[s, 0])
            vo_ref[s, 0] = vv
            return acc + vv.astype(F32) * sc_ref[pl.ds(s, 1), :]
        acc = lax.fori_loop(0, slots, values, jnp.zeros(k_new.shape, F32), unroll=4)
        attn_ref[...] = acc.astype(BF16)


def whole_row_norm(h, gain, shift):
    mean = jnp.mean(h, axis=-1, keepdims=True)
    dev = h - mean
    var = jnp.mean(dev * dev, axis=-1, keepdims=True)
    return (dev * lax.rsqrt(var + LN_EPS) * gain + shift).astype(BF16)


def mlp_kernel(attn_ref, w0_ref, w1_ref, w2_ref, w3_ref, hres_ref, vecs_ref, bup_ref,
               out_ref,
               wg, wv, wd, wo, p1, s1d, r1d, s1y, r1y, zfull,
               keep, sd, rd, sy, ry, sz, rz, ob, ofull,
               a_s, a_r, zz_s, zz_r, zy_s, zy_r, zd_s, zd_r,
               md_s, md_r, my_s, my_r, mz_s, mz_r, oz_s, oz_r, oy_s, oy_r, od_s, od_r):
    dp, x, y, core, chip, piece = where_am_i()
    mate = (dp, x, chip * 2 + 1 - core)
    across = (dp, x, (1 - chip) * 2 + core)
    peers = [(dp, lax.rem(x + j, 4), y) for j in (1, 2, 3)]
    source = [lax.rem(x + 4 - j, 4) for j in (0, 1, 2, 3)]
    sends = []

    def go(src, dst, send, recv, device):
        c = remote(src, dst, send, recv, device)
        c.start()
        sends.append(c)
        return c

    greet(peers + [mate, across])
    for j, ref in enumerate((w0_ref, w1_ref, w2_ref, w3_ref)):
        at = pl.ds(pl.multiple_of(source[j] * 256, 256), 256)
        wg[at, :] = ref[0:256, :]
        wv[at, :] = ref[256:512, :]
        wd[:, at] = ref[512:768, :]
        wo[:, at] = ref[768:1024, :]

    mine = attn_ref[:, pl.ds(pl.multiple_of(x * 256, 256), 256)].astype(F32).T.astype(BF16)
    p1[...] = jnp.dot(mine, wo[...], preferred_element_type=F32)
    s1d[...] = p1[pl.ds(pl.multiple_of((1 - core) * 128, 128), 128), :].astype(BF16)
    c = go(s1d, r1d, a_s.at[0], a_r.at[0], mate)
    c.wait_recv()
    give = (1 - chip) * 64
    hold = chip * 64
    base = core * 128
    s1y[...] = (p1[pl.ds(pl.multiple_of(base + give, 64), 64), :]
                + r1d[pl.ds(pl.multiple_of(give, 64), 64), :].astype(F32)).astype(BF16)
    c = go(s1y, r1y, a_s.at[1], a_r.at[1], across)
    h = (p1[pl.ds(pl.multiple_of(base + hold, 64), 64), :]
         + r1d[pl.ds(pl.multiple_of(hold, 64), 64), :].astype(F32))
    c.wait_recv()
    h = h + r1y[...].astype(F32)
    h = DEEP_ALPHA * hres_ref[...].astype(F32) + (h + vecs_ref[0:1, :])
    zfull[x, piece] = whole_row_norm(h, vecs_ref[1:2, :], vecs_ref[2:3, :])

    own = zfull.at[x, piece]
    zz = [go(own, own, zz_s.at[j], zz_r.at[j], peers[j - 1]) for j in (1, 2, 3)]
    zy = [go(own, own, zy_s.at[0], zy_r.at[0], across)]
    for j in (1, 2, 3):
        zz[j - 1].wait_recv()
        block = zfull.at[source[j], piece]
        zy.append(go(block, block, zy_s.at[j], zy_r.at[j], across))
        if j == 1:
            zy[0].wait_recv()
            both = zfull.at[x, pl.ds(core * 2, 2)]
            zd = [go(both, both, zd_s.at[0], zd_r.at[0], mate)]

    def mlp(j):
        z = zfull[source[j]].reshape(256, 1024)
        gate = jnp.dot(z, wg[...], preferred_element_type=F32) + bup_ref[0:1, :]
        value = jnp.dot(z, wv[...], preferred_element_type=F32) + bup_ref[1:2, :]
        g = (jax.nn.gelu(gate, approximate=True) * value).astype(BF16)
        p1[...] = jnp.dot(g, wd[...], preferred_element_type=F32)
        sd[j] = p1[pl.ds(pl.multiple_of((1 - core) * 128, 128), 128), :].astype(BF16)
        keep[j] = p1[pl.ds(pl.multiple_of(base, 128), 128), :]
        return go(sd.at[j], rd.at[j], md_s.at[j], md_r.at[j], mate)

    def pair_sum(j, c):
        c.wait_recv()
        at = pl.ds(pl.multiple_of(give, 64), 64)
        sy[j] = (keep[j, at, :] + rd[j, at, :].astype(F32)).astype(BF16)
        return go(sy.at[j], ry.at[j], my_s.at[j], my_r.at[j], across)

    def chip_sum(j, c):
        c.wait_recv()
        at = pl.ds(pl.multiple_of(hold, 64), 64)
        total = keep[j, at, :] + rd[j, at, :].astype(F32) + ry[j].astype(F32)
        if j == 0:
            keep[0, 0:64, :] = total
            return None
        sz[j] = total.astype(BF16)
        back = (dp, source[j], y)
        return go(sz.at[j], rz.at[j], mz_s.at[j], mz_r.at[j], back)

    md, my, mz = {}, {}, {}
    for t in range(6):
        if t < 4:
            if t > 0:
                zy[t].wait_recv()
                both = zfull.at[source[t], pl.ds(core * 2, 2)]
                zd.append(go(both, both, zd_s.at[t], zd_r.at[t], mate))
            zd[t].wait_recv()
            md[t] = mlp(t)
        if 1 <= t < 5:
            my[t - 1] = pair_sum(t - 1, md[t - 1])
        if 2 <= t:
            mz[t - 2] = chip_sum(t - 2, my[t - 2])
    h = keep[0, 0:64, :]
    for j in (1, 2, 3):
        mz[j].wait_recv()
        h = h + rz[j].astype(F32)
    h = DEEP_ALPHA * zfull[x, piece].astype(F32) + h + vecs_ref[3:4, :]
    o = whole_row_norm(h, vecs_ref[4:5, :], vecs_ref[5:6, :])

    for s in range(4):
        ob[s] = o[:, s * 256:(s + 1) * 256]
    ofull[x, piece] = ob[x]
    oz = [go(ob.at[lax.rem(x + j, 4)], ofull.at[x, piece], oz_s.at[j], oz_r.at[j], peers[j - 1]) for j in (1, 2, 3)]
    oy = []
    for j in range(4):
        if j > 0:
            oz[j - 1].wait_recv()
        block = ofull.at[source[j], piece]
        oy.append(go(block, block, oy_s.at[j], oy_r.at[j], across))
    od = []
    for j in range(4):
        oy[j].wait_recv()
        both = ofull.at[source[j], pl.ds(core * 2, 2)]
        od.append(go(both, both, od_s.at[j], od_r.at[j], mate))
    for c in od:
        c.wait_recv()
    out_ref[...] = ofull[...].reshape(1024, 256)
    for c in sends:
        c.wait_send()


def solution(mesh):
    cache_spec = P('dp', None, 'y', None)
    width_spec = P('x')
    in_specs = (P('dp', 'x'), P('x', 'y'), P('y'), P('y', 'x'), width_spec, width_spec, width_spec, P('x', None, 'y'), P(None, 'y'), P('y', 'x'), width_spec, width_spec, width_spec, cache_spec, cache_spec, P('dp'), P('dp'))
    out_specs = (P('dp', 'x'), cache_spec, cache_spec)
    vmem = pl.BlockSpec(memory_space=VMEM)
    dma = pltpu.SemaphoreType.DMA

    def local_step(hidden, w_qkv, b_qkv, w_out, b_out, attn_gain, attn_shift, w_up, b_up, w_down, b_down, mlp_gain, mlp_shift, k_cache, v_cache, positions, lengths):
        x = lax.axis_index('x')
        inv_freq = ROPE_BASE ** (-2.0 * jnp.arange(32, dtype=F32) / 64)
        angles = inv_freq[:, None] * positions.astype(F32)[None, :]
        cos, sin = jnp.cos(angles), jnp.sin(angles)
        vec = jnp.stack([v.astype(F32) for v in (b_out, attn_gain, attn_shift, b_down, mlp_gain, mlp_shift, b_out, b_out)])
        row = jax.ShapeDtypeStruct((256, 1024), BF16)
        q, k_new, v_new, hres, vecs = pl.pallas_call(
            qkv_kernel,
            name="gather_qkv",
            out_shape=(row, row, row, jax.ShapeDtypeStruct((64, 1024), BF16), jax.ShapeDtypeStruct((8, 1024), F32)),
            in_specs=[vmem] * 6,
            out_specs=(vmem,) * 5,
            scratch_shapes=[
                VMEM((4, 4, 256, 256), BF16),
                VMEM((4, 2, 128, 768), BF16),
                VMEM((4, 8, 256), F32),
            ] + [dma((4,))] * 12,
            compiler_params=pltpu.CompilerParams(collective_id=0, has_side_effects=True),
            cost_estimate=pl.CostEstimate(flops=2 * 1024 * 1024 * 768, bytes_accessed=8 << 20, transcendentals=0),
        )(hidden, w_qkv, b_qkv.reshape(1, 768), vec, cos, sin)

        packs = []
        for j in range(4):
            t = lax.rem(x + j, 4) * 256
            up = lax.dynamic_slice_in_dim(w_up, t, 256, axis=2)
            down = lax.dynamic_slice_in_dim(w_down, t, 256, axis=0)
            packs.append(jnp.concatenate([up[:, 0], up[:, 1], down, w_out], axis=0))
        q, *packs = lax.optimization_barrier((q, *packs))
        moved = [packs[0]] + [lax.ppermute(packs[j], 'x', [(i, (i + j) % 4) for i in range(4)]) for j in (1, 2, 3)]
        bup = lax.dynamic_slice_in_dim(b_up, x * 256, 256, axis=1).astype(F32)

        k_t, v_t = k_cache.transpose(1, 2, 3, 0), v_cache.transpose(1, 2, 3, 0)
        big = pl.BlockSpec((64, 1, 64, 256), lambda r, h: (0, h, 0, r))
        small = pl.BlockSpec((64, 256), lambda r, h: (h, r))
        k_full, v_full, attn = pl.pallas_call(
            cache_kernel,
            name="cache_attend",
            grid=(4, 4),
            out_shape=(jax.ShapeDtypeStruct(k_t.shape, BF16), jax.ShapeDtypeStruct(v_t.shape, BF16), row),
            in_specs=[pl.BlockSpec((1, 256), lambda r, h: (0, r)), small, small, small, big, big],
            out_specs=(big, big, small),
            scratch_shapes=[VMEM((64, 256), F32)],
            cost_estimate=pl.CostEstimate(flops=4 * 10 ** 9, bytes_accessed=128 << 20, transcendentals=0),
        )(lengths.reshape(1, 1024), q, k_new, v_new, k_t, v_t)

        out = pl.pallas_call(
            mlp_kernel,
            name="project_mlp",
            out_shape=jax.ShapeDtypeStruct((1024, 256), BF16),
            in_specs=[vmem] * 8,
            out_specs=vmem,
            scratch_shapes=[
                VMEM((1024, 256), BF16), VMEM((1024, 256), BF16), VMEM((256, 1024), BF16), VMEM((256, 1024), BF16),
                VMEM((256, 1024), F32),
                VMEM((128, 1024), BF16), VMEM((128, 1024), BF16), VMEM((64, 1024), BF16), VMEM((64, 1024), BF16),
                VMEM((4, 4, 64, 1024), BF16),
                VMEM((4, 128, 1024), F32),
                VMEM((4, 128, 1024), BF16), VMEM((4, 128, 1024), BF16),
                VMEM((4, 64, 1024), BF16), VMEM((4, 64, 1024), BF16),
                VMEM((4, 64, 1024), BF16), VMEM((4, 64, 1024), BF16),
                VMEM((4, 64, 256), BF16),
                VMEM((4, 4, 64, 256), BF16),
            ] + [dma((4,))] * 20,
            compiler_params=pltpu.CompilerParams(collective_id=1, has_side_effects=True),
            cost_estimate=pl.CostEstimate(flops=4 * 10 ** 9, bytes_accessed=8 << 20, transcendentals=0),
        )(attn, *moved, hres, vecs, bup)
        return out, k_full.transpose(3, 0, 1, 2), v_full.transpose(3, 0, 1, 2)

    return jax.shard_map(local_step, mesh=mesh, in_specs=in_specs, out_specs=out_specs, check_vma=False)
```

```python
import functools
import math
import jax
import jax.numpy as jnp
from jax import lax
from jax.experimental import pallas as pl
from jax.experimental.pallas import tpu as pltpu
from jax.sharding import PartitionSpec as P

DEEP_ALPHA = math.sqrt(140.0)
LN_EPS = 1e-5
ROPE_BASE = 10000.0
MESH = pl.DeviceIdType.MESH
VMEM = pltpu.VMEM
F32 = jnp.float32
BF16 = jnp.bfloat16
N = 4
OTHERS = range(1, N)
HEAD = 64
HALF = HEAD // 2
PART = N * HEAD
PAIR = PART // 2
WIDE = N * PART


def where_am_i():
    dp, x, y = lax.axis_index("dp"), lax.axis_index("x"), lax.axis_index("y")
    core, chip = lax.rem(y, 2), y // 2
    return dp, x, y, core, chip, core * 2 + chip


def remote(src, dst, send, recv, device):
    return pltpu.make_async_remote_copy(
        src_ref=src, dst_ref=dst, send_sem=send, recv_sem=recv, device_id=device, device_id_type=MESH)


def greet(devices):
    barrier = pltpu.get_barrier_semaphore()
    for device in devices:
        pl.semaphore_signal(barrier, inc=1, device_id=device, device_id_type=MESH)
    pl.semaphore_wait(barrier, len(devices))


def qkv_kernel(hid_ref, w_ref, b_ref, bo_ref, ag_ref, as_ref, bd_ref, mg_ref, ms_ref, pos_ref, up_ref, down_ref, wout_ref, vc_ref,
               q_ref, k_ref, v_ref, hres_ref, vecs_ref, p0_ref, p1_ref, p2_ref, p3_ref, vres_ref,
               hbuf, wbuf, vbuf, vrow, acc_ref, cos_ref, sin_ref, hr_s, hl_s, h_r, hy_s, hy_r, hd_s, hd_r, wr_s, wl_s, w_r, wx_s, wx_r, vz_s, vz_r, pre_s):
    dp, x, y, core, chip, piece = where_am_i()
    mate = (dp, x, chip * 2 + 1 - core)
    across = (dp, x, (1 - chip) * 2 + core)
    twin = (1 - dp, x, y)
    peers = [(dp, lax.rem(x + j, N), y) for j in OTHERS]
    source = [lax.rem(x + N - j, N) for j in range(N)]
    right, left = peers[0], peers[2]
    fetch = pltpu.make_async_copy(vc_ref.at[pl.ds(0, RESIDENT)], vres_ref, pre_s)
    fetch.start()
    for n, ref in enumerate((bo_ref, ag_ref, as_ref, bd_ref, mg_ref, ms_ref)):
        vrow[n:n + 1, :] = ref[...].astype(F32).reshape(1, PART)
    vrow[6:8, :] = jnp.zeros((2, 256), F32)
    greet(peers + [mate, across, twin])

    row0 = pl.multiple_of(piece * PART, PART)
    half0 = pl.multiple_of(dp * PAIR, PAIR)
    own_h, own_w = hid_ref.at[pl.ds(row0, 256)], w_ref.at[pl.ds(half0, 128)]

    def h_move(src, s, k, to_right):
        return remote(src, hbuf.at[piece, s], (hr_s if to_right else hl_s).at[k], h_r.at[s], right if to_right else left)

    def w_move(src, s, k, to_right):
        return remote(src, wbuf.at[s, dp], (wr_s if to_right else wl_s).at[k], w_r.at[s], right if to_right else left)

    def y_move(s):
        return remote(hbuf.at[piece, s], hbuf.at[piece, s], hy_s.at[s], hy_r.at[s], across)

    def d_move(s):
        both = hbuf.at[pl.ds(core * 2, 2), s]
        return remote(both, both, hd_s.at[s], hd_r.at[s], mate)

    def x_move(s):
        return remote(wbuf.at[s, dp], wbuf.at[s, dp], wx_s.at[s], wx_r.at[s], twin)

    def sides(k, act):
        @pl.when(x >= k)
        def _():
            act(lax.max(x - k, 0), True)

        @pl.when(x + k <= 3)
        def _():
            act(lax.min(x + k, 3), False)

    def onward(k, act):
        for to_right, at in ((True, x), (False, 3 - x)):
            @pl.when((at - k) * (2 - at) >= 0)
            def _():
                act(lax.max(x - k, 0) if to_right else lax.min(x + k, 3), to_right)

    def start_own(s, to_right):
        h_move(own_h, x, 0, to_right).start()
        w_move(own_w, x, 0, to_right).start()

    def sent_own(s, to_right):
        h_move(own_h, x, 0, to_right).wait_send()
        w_move(own_w, x, 0, to_right).wait_send()

    onward(0, start_own)
    vz = []
    for j in OTHERS:
        c = remote(vrow, vbuf.at[x], vz_s.at[j], vz_r.at[j], peers[j - 1])
        c.start()
        vz.append(c)
    vbuf[x] = vrow[...]
    for part in range(N):
        hbuf[part, x] = hid_ref[part * PART:(part + 1) * PART, :]
    for half in range(2):
        wbuf[x, half] = w_ref[half * PAIR:(half + 1) * PAIR, :]

    for k in OTHERS:
        def arrive_h(s, to_right):
            h_move(hbuf.at[piece, s], s, k, to_right).wait_recv()
            y_move(s).start()

        def arrive_w(s, to_right):
            w_move(wbuf.at[s, dp], s, k, to_right).wait_recv()
            x_move(s).start()

        def arrive_y(s, to_right):
            y_move(s).wait_recv()
            d_move(s).start()

        sides(k, arrive_h)
        if k < 3:
            onward(k, lambda s, to_right: h_move(hbuf.at[piece, s], s, k, to_right).start())
        sides(k, arrive_w)
        if k < 3:
            onward(k, lambda s, to_right: w_move(wbuf.at[s, dp], s, k, to_right).start())
        sides(k, arrive_y)
        if k == 1:
            def own_rows(part, _):
                at = pl.ds(pl.multiple_of(part * PART, PART), 256)
                acc_ref[at, :] = jnp.dot(hid_ref[at, :], w_ref[...], preferred_element_type=F32)
                return 0

            lax.fori_loop(0, N, own_rows, 0)
        if k == 2:
            for j, ref in enumerate((p0_ref, p1_ref, p2_ref, p3_ref)):
                at = pl.ds(pl.multiple_of(lax.rem(x + j, N) * PART, PART), 256)
                ref[0:PART, :] = up_ref[:, 0, at]
                ref[PART:2 * PART, :] = up_ref[:, 1, at]
                ref[2 * PART:3 * PART, :] = down_ref[at, :]
                ref[3 * PART:, :] = wout_ref[...]
            half_dim = lax.broadcasted_iota(jnp.int32, (HALF, WIDE), 0).astype(F32)
            angles = jnp.exp(half_dim * (-2.0 / 64 * math.log(ROPE_BASE))) * pos_ref[...].astype(F32)
            cos_all, sin_all = jnp.cos(angles), jnp.sin(angles)
            cos_ref[...] = cos_all
            sin_ref[...] = sin_all
    far = x // 2
    order = [1 - x + N * far, 2 - far, 3 * (1 - far)]
    for n, s in enumerate(order):
        d_move(s).wait_recv()
        x_move(s).wait_recv()
        vz[n].wait_recv()
        if n < 2:
            def add_rows(part, _):
                at = pl.ds(pl.multiple_of(part * PART, PART), PART)
                acc_ref[at, :] += jnp.dot(hbuf[part, s], wbuf[s].reshape(PART, -1), preferred_element_type=F32)
                return 0

            lax.fori_loop(0, N, add_rows, 0)

    for s in range(N):
        hres_ref[:, s * PART:(s + 1) * PART] = hbuf[x, s, pl.ds(pl.multiple_of(piece * HEAD, HEAD), 64), :]
        vecs_ref[:, s * PART:(s + 1) * PART] = vbuf[s]

    def rows(part, _):
        lanes = pl.ds(pl.multiple_of(part * PART, PART), 256)
        acc = acc_ref[lanes, :]
        acc += jnp.dot(hbuf[part, order[2]], wbuf[order[2]].reshape(PART, -1), preferred_element_type=F32)
        acc = (acc + b_ref[...].astype(F32).reshape(1, -1)).astype(BF16).astype(F32)
        cos, sin = cos_ref[:, lanes], sin_ref[:, lanes]
        acc = acc.T
        for head in range(N):
            base = head * 192
            for off, ref in ((0, q_ref), (64, k_ref)):
                low, high = acc[base + off:base + off + 32], acc[base + off + 32:base + off + 64]
                ref[head * 64:head * 64 + 32, lanes] = (low * cos - high * sin).astype(BF16)
                ref[head * 64 + 32:head * 64 + 64, lanes] = (high * cos + low * sin).astype(BF16)
            v_ref[head * HEAD:(head + 1) * HEAD, lanes] = acc[base + 128:base + 192].astype(BF16)
        return 0

    lax.fori_loop(0, N, rows, 0)
    onward(0, sent_own)
    for k in (1, 2):
        def sent(s, to_right):
            h_move(hbuf.at[piece, s], s, k, to_right).wait_send()
            w_move(wbuf.at[s, dp], s, k, to_right).wait_send()
        onward(k, sent)
    for j in OTHERS:
        vz[j - 1].wait_send()
        y_move(source[j]).wait_send()
        d_move(source[j]).wait_send()
        x_move(source[j]).wait_send()
    fetch.wait()


TILE = 2
DEPTH = 8
ROOM = 44 << 20
RESIDENT = 32


def cache_kernel(len_ref, q_ref, kn_ref, vn_ref, vres_ref, k_ref, v_ref, ko_ref, vo_ref, attn_ref,
                 ibuf, obuf, lens_b, q_own, sc_ref, acc_ref, in_sem, out_sem):
    slots = k_ref.shape[0]
    tiles = slots // TILE
    held = RESIDENT // TILE
    own = pl.ds(pl.multiple_of(lax.axis_index("x") * PART, PART), 256)

    def fetch(ref, t, slot):
        return pltpu.make_async_copy(ref.at[pl.ds(t * TILE, TILE)], ibuf.at[slot], in_sem.at[slot])

    def flush(ref, t, slot):
        return pltpu.make_async_copy(obuf.at[slot], ref.at[pl.ds(t * TILE, TILE)], out_sem.at[slot])

    for t in range(DEPTH):
        fetch(k_ref, t, t).start()
    lens_b[...] = jnp.broadcast_to(len_ref[...].astype(F32), lens_b.shape).astype(BF16)
    q_own[...] = q_ref[:, own].astype(F32)

    def update(slot, i, s, new_ref, old_ref):
        hit = lens_b[...] == jnp.full(lens_b.shape, s.astype(F32), F32).astype(BF16)
        hit = jnp.broadcast_to(hit[None], (16, 16, WIDE))
        old = old_ref[...].reshape(16, 16, WIDE)
        new = new_ref[...].reshape(16, 16, WIDE)
        obuf[slot, i] = jnp.where(hit, new, old).reshape(N, HEAD, WIDE)

    def keys(t, _):
        slot = lax.rem(t, DEPTH)
        fetch(k_ref, t, slot).wait()

        @pl.when(t >= DEPTH)
        def _():
            flush(ko_ref, t - DEPTH, slot).wait()
        for i in range(TILE):
            update(slot, i, t * TILE + i, kn_ref, ibuf.at[slot, i])
        flush(ko_ref, t, slot).start()

        @pl.when(t < tiles - DEPTH)
        def _():
            fetch(k_ref, t + DEPTH, slot).start()

        @pl.when(t >= tiles - DEPTH)
        def _():
            fetch(v_ref, held + t + DEPTH - tiles, slot).start()
        for i in range(TILE):
            for head in range(N):
                prod = obuf[slot, i, head, :, own].astype(F32) * q_own[head * HEAD:(head + 1) * HEAD, :]
                sc_ref[head, pl.ds(t * TILE + i, 1), :] = jnp.sum(prod, axis=0, keepdims=True)
        return 0

    lax.fori_loop(0, tiles, keys, 0)
    sc = sc_ref[...] * (HEAD ** -0.5)
    valid = lax.broadcasted_iota(jnp.int32, sc.shape, 1) <= jnp.broadcast_to(len_ref[:, own][None], sc.shape)
    sc = jnp.where(valid, sc, -1e30)
    e = jnp.exp(sc - jnp.max(sc, axis=1, keepdims=True))
    sc_ref[...] = (e / jnp.sum(e, axis=1, keepdims=True)).astype(BF16).astype(F32)
    acc_ref[...] = jnp.zeros_like(acc_ref)

    def weigh(slot, t):
        for head in range(N):
            at = slice(head * HEAD, (head + 1) * HEAD)
            part = acc_ref[at, :]
            for i in range(TILE):
                part += obuf[slot, i, head, :, own].astype(F32) * sc_ref[head, pl.ds(t * TILE + i, 1), :]
            acc_ref[at, :] = part

    def values(n, _):
        slot, t = lax.rem(n, DEPTH), held + n
        fetch(v_ref, t, slot).wait()

        @pl.when(n >= DEPTH)
        def _():
            flush(vo_ref, t - DEPTH, slot).wait()

        @pl.when(n < DEPTH)
        def _():
            flush(ko_ref, n + tiles - DEPTH, slot).wait()
        for i in range(TILE):
            update(slot, i, t * TILE + i, vn_ref, ibuf.at[slot, i])
        flush(vo_ref, t, slot).start()

        @pl.when(n < tiles - held - DEPTH)
        def _():
            fetch(v_ref, t + DEPTH, slot).start()
        weigh(slot, t)
        return 0

    def held_values(t, _):
        slot = lax.rem(t, DEPTH)
        flush(vo_ref, t, slot).wait()
        for i in range(TILE):
            update(slot, i, t * TILE + i, vn_ref, vres_ref.at[t * TILE + i])
        flush(vo_ref, t, slot).start()
        weigh(slot, t)
        return 0

    lax.fori_loop(0, tiles - held, values, 0)
    lax.fori_loop(0, held, held_values, 0)
    attn_ref[...] = acc_ref[...].astype(BF16)
    for slot in range(DEPTH):
        flush(vo_ref, slot, slot).wait()


def whole_row_norm(h, gain, shift):
    mean = jnp.mean(h, axis=-1, keepdims=True)
    dev = h - mean
    var = jnp.mean(dev * dev, axis=-1, keepdims=True)
    return (dev * lax.rsqrt(var + LN_EPS) * gain + shift).astype(BF16)


def mlp_kernel(attn_ref, w0_ref, w1_ref, w2_ref, w3_ref, hres_ref, vecs_ref, bup_ref,
               out_ref,
               wg, wv, wd, wo, p1, s1d, r1d, s1y, r1y, zfull,
               keep, sd, rd, sy, ry, sz, rz, ob, ofull,
               a_s, a_r, zz_s, zz_r, zy_s, zy_r, zd_s, zd_r,
               md_s, md_r, my_s, my_r, mz_s, mz_r, oz_s, oz_r, oy_s, oy_r, od_s, od_r):
    dp, x, y, core, chip, piece = where_am_i()
    mate = (dp, x, chip * 2 + 1 - core)
    across = (dp, x, (1 - chip) * 2 + core)
    peers = [(dp, lax.rem(x + j, N), y) for j in OTHERS]
    source = [lax.rem(x + N - j, N) for j in range(N)]
    sends = []

    def go(src, dst, send, recv, device):
        c = remote(src, dst, send, recv, device)
        c.start()
        sends.append(c)
        return c

    greet(peers + [mate, across])
    bup = bup_ref[:, pl.ds(pl.multiple_of(x * PART, PART), 256)].astype(F32)
    columns = [pl.ds(pl.multiple_of(source[j] * PART, PART), 256) for j in range(N)]
    packs = (w0_ref, w1_ref, w2_ref, w3_ref)
    for j in range(N):
        wo[:, columns[j]] = packs[j][3 * PART:, :]

    mine = attn_ref[...].astype(F32).T.astype(BF16)
    p1[...] = jnp.dot(mine, wo[...], preferred_element_type=F32)
    s1d[...] = p1[pl.ds(pl.multiple_of((1 - core) * PAIR, PAIR), 128), :].astype(BF16)
    c = go(s1d, r1d, a_s.at[0], a_r.at[0], mate)
    for j in range(N):
        wd[:, columns[j]] = packs[j][2 * PART:3 * PART, :]
    c.wait_recv()
    give = (1 - chip) * 64
    hold = chip * 64
    base = core * 128
    s1y[...] = (p1[pl.ds(pl.multiple_of(base + give, HEAD), HEAD), :]
                + r1d[pl.ds(pl.multiple_of(give, HEAD), HEAD), :].astype(F32)).astype(BF16)
    c = go(s1y, r1y, a_s.at[1], a_r.at[1], across)
    h = (p1[pl.ds(pl.multiple_of(base + hold, HEAD), HEAD), :]
         + r1d[pl.ds(pl.multiple_of(hold, HEAD), HEAD), :].astype(F32))
    for j in range(N):
        wg[columns[j], :] = packs[j][0:PART, :]
        wv[columns[j], :] = packs[j][PART:2 * PART, :]
    c.wait_recv()
    h = h + r1y[...].astype(F32)
    h = DEEP_ALPHA * hres_ref[...].astype(F32) + (h + vecs_ref[0:1, :])
    zfull[x, piece] = whole_row_norm(h, vecs_ref[1:2, :], vecs_ref[2:3, :])

    own = zfull.at[x, piece]
    zz = [go(own, own, zz_s.at[j], zz_r.at[j], peers[j - 1]) for j in OTHERS]
    zy = [go(own, own, zy_s.at[0], zy_r.at[0], across)]
    for j in OTHERS:
        zz[j - 1].wait_recv()
        block = zfull.at[source[j], piece]
        zy.append(go(block, block, zy_s.at[j], zy_r.at[j], across))
        if j == 1:
            zy[0].wait_recv()
            both = zfull.at[x, pl.ds(core * 2, 2)]
            zd = [go(both, both, zd_s.at[0], zd_r.at[0], mate)]

    def mlp(j):
        z = zfull[source[j]].reshape(PART, WIDE)
        gate = jnp.dot(z, wg[...], preferred_element_type=F32) + bup[0:1, :]
        value = jnp.dot(z, wv[...], preferred_element_type=F32) + bup[1:2, :]
        g = (jax.nn.gelu(gate, approximate=True) * value).astype(BF16)
        p1[...] = jnp.dot(g, wd[...], preferred_element_type=F32)
        sd[j] = p1[pl.ds(pl.multiple_of((1 - core) * PAIR, PAIR), 128), :].astype(BF16)
        keep[j] = p1[pl.ds(pl.multiple_of(base, 128), 128), :]
        return go(sd.at[j], rd.at[j], md_s.at[j], md_r.at[j], mate)

    def pair_sum(j, c):
        c.wait_recv()
        at = pl.ds(pl.multiple_of(give, HEAD), HEAD)
        sy[j] = (keep[j, at, :] + rd[j, at, :].astype(F32)).astype(BF16)
        return go(sy.at[j], ry.at[j], my_s.at[j], my_r.at[j], across)

    def chip_sum(j, c):
        c.wait_recv()
        at = pl.ds(pl.multiple_of(hold, HEAD), HEAD)
        total = keep[j, at, :] + rd[j, at, :].astype(F32) + ry[j].astype(F32)
        if j == 0:
            keep[0, 0:64, :] = total
            return None
        sz[j] = total.astype(BF16)
        back = (dp, source[j], y)
        return go(sz.at[j], rz.at[j], mz_s.at[j], mz_r.at[j], back)

    my, mz = {}, {}
    for t in range(N):
        zd[t].wait_recv()
        c = mlp(t)
        if t < 3:
            zy[t + 1].wait_recv()
            both = zfull.at[source[t + 1], pl.ds(core * 2, 2)]
            zd.append(go(both, both, zd_s.at[t + 1], zd_r.at[t + 1], mate))
        my[t] = pair_sum(t, c)
        if t > 0:
            mz[t - 1] = chip_sum(t - 1, my[t - 1])
    mz[3] = chip_sum(3, my[3])
    h = keep[0, 0:64, :]
    for j in OTHERS:
        mz[j].wait_recv()
        h = h + rz[j].astype(F32)
    h = DEEP_ALPHA * zfull[x, piece].astype(F32) + h + vecs_ref[3:4, :]
    o = whole_row_norm(h, vecs_ref[4:5, :], vecs_ref[5:6, :])

    for s in range(N):
        ob[s] = o[:, s * PART:(s + 1) * PART]
    ofull[x, piece] = ob[x]
    oz = [go(ob.at[lax.rem(x + j, N)], ofull.at[x, piece], oz_s.at[j], oz_r.at[j], peers[j - 1]) for j in OTHERS]
    oy = []
    for j in range(N):
        if j > 0:
            oz[j - 1].wait_recv()
        block = ofull.at[source[j], piece]
        oy.append(go(block, block, oy_s.at[j], oy_r.at[j], across))
    od = []
    for j in range(N):
        oy[j].wait_recv()
        both = ofull.at[source[j], pl.ds(core * 2, 2)]
        od.append(go(both, both, od_s.at[j], od_r.at[j], mate))
    for c in od:
        c.wait_recv()
    out_ref[...] = ofull[...].reshape(WIDE, PART)
    for c in sends:
        c.wait_send()


def solution(mesh):
    cache_spec = P('dp', None, 'y', None)
    width_spec = P('x')
    in_specs = (P('dp', 'x'), P('x', 'y'), P('y'), P('y', 'x'), width_spec, width_spec, width_spec, P('x', None, 'y'), P(None, 'y'), P('y', 'x'), width_spec, width_spec, width_spec, cache_spec, cache_spec, P('dp'), P('dp'))
    out_specs = (P('dp', 'x'), cache_spec, cache_spec)
    vmem = pl.BlockSpec(memory_space=VMEM)
    dma = pltpu.SemaphoreType.DMA

    def local_step(hidden, w_qkv, b_qkv, w_out, b_out, attn_gain, attn_shift, w_up, b_up, w_down, b_down, mlp_gain, mlp_shift, k_cache, v_cache, positions, lengths):
        k_t, v_t = k_cache.transpose(1, 2, 3, 0), v_cache.transpose(1, 2, 3, 0)
        anywhere = pl.BlockSpec(memory_space=pl.ANY)
        row = jax.ShapeDtypeStruct((PART, WIDE), BF16)
        pack = jax.ShapeDtypeStruct((WIDE, PART), BF16)
        q, k_new, v_new, hres, vecs, *packs, v_res = pl.pallas_call(
            qkv_kernel,
            name="gather_qkv",
            out_shape=(row, row, row, jax.ShapeDtypeStruct((HEAD, WIDE), BF16), jax.ShapeDtypeStruct((8, WIDE), F32)) + (pack,) * 4 + (VMEM((RESIDENT, N, HEAD, WIDE), BF16),),
            in_specs=[vmem] * 13 + [anywhere],
            out_specs=(vmem,) * 10,
            scratch_shapes=[
                VMEM((N, N, PART, PART), BF16),
                VMEM((4, 2, 128, 768), BF16),
                VMEM((N, 8, PART), F32),
                VMEM((8, PART), F32),
                VMEM((1024, 768), F32),
                VMEM((HALF, WIDE), F32),
                VMEM((HALF, WIDE), F32),
            ] + [dma((N,))] * 14 + [dma(())],
            compiler_params=pltpu.CompilerParams(collective_id=0, has_side_effects=True, vmem_limit_bytes=ROOM),
            cost_estimate=pl.CostEstimate(flops=2 * 1024 * 1024 * 768, bytes_accessed=8 << 20, transcendentals=0),
        )(hidden, w_qkv, b_qkv, b_out, attn_gain, attn_shift, b_down, mlp_gain, mlp_shift, positions.reshape(1, WIDE), w_up, w_down, w_out, v_t)

        moved = [packs[0]] + [lax.ppermute(packs[j], 'x', [(i, (i + j) % 4) for i in range(N)]) for j in OTHERS]

        k_full, v_full, attn = pl.pallas_call(
            cache_kernel,
            name="cache_attend",
            out_shape=(jax.ShapeDtypeStruct(k_t.shape, BF16), jax.ShapeDtypeStruct(v_t.shape, BF16), jax.ShapeDtypeStruct((PART, PART), BF16)),
            in_specs=[vmem] * 5 + [anywhere] * 2,
            out_specs=(anywhere, anywhere, vmem),
            scratch_shapes=[
                VMEM((DEPTH, TILE, N, HEAD, WIDE), BF16), VMEM((DEPTH, TILE, N, HEAD, WIDE), BF16),
                VMEM((16, 1024), BF16), VMEM((PART, PART), F32), VMEM((N, HEAD, PART), F32), VMEM((PART, PART), F32),
                dma((DEPTH,)), dma((DEPTH,)),
            ],
            compiler_params=pltpu.CompilerParams(vmem_limit_bytes=ROOM),
            cost_estimate=pl.CostEstimate(flops=4 * 10 ** 9, bytes_accessed=128 << 20, transcendentals=0),
        )(lengths.reshape(1, WIDE), q, k_new, v_new, pltpu.with_memory_space_constraint(v_res, VMEM), k_t, v_t)

        out = pl.pallas_call(
            mlp_kernel,
            name="project_mlp",
            out_shape=jax.ShapeDtypeStruct((WIDE, PART), BF16),
            in_specs=[vmem] * 8,
            out_specs=vmem,
            scratch_shapes=[
                VMEM((WIDE, PART), BF16), VMEM((WIDE, PART), BF16), VMEM((PART, WIDE), BF16), VMEM((PART, WIDE), BF16),
                VMEM((PART, WIDE), F32),
                VMEM((PAIR, WIDE), BF16), VMEM((PAIR, WIDE), BF16), VMEM((HEAD, WIDE), BF16), VMEM((HEAD, WIDE), BF16),
                VMEM((N, N, HEAD, WIDE), BF16),
                VMEM((N, PAIR, WIDE), F32),
                VMEM((N, PAIR, WIDE), BF16), VMEM((N, PAIR, WIDE), BF16),
                VMEM((N, HEAD, WIDE), BF16), VMEM((N, HEAD, WIDE), BF16),
                VMEM((N, HEAD, WIDE), BF16), VMEM((N, HEAD, WIDE), BF16),
                VMEM((N, HEAD, PART), BF16),
                VMEM((N, N, HEAD, PART), BF16),
            ] + [dma((N,))] * 20,
            compiler_params=pltpu.CompilerParams(collective_id=1, has_side_effects=True, vmem_limit_bytes=ROOM),
            cost_estimate=pl.CostEstimate(flops=4 * 10 ** 9, bytes_accessed=8 << 20, transcendentals=0),
        )(attn, *moved, hres, vecs, b_up)
        return out, k_full.transpose(3, 0, 1, 2), v_full.transpose(3, 0, 1, 2)

    return jax.shard_map(local_step, mesh=mesh, in_specs=in_specs, out_specs=out_specs, check_vma=False)
```
